32 devices in a mesh: member: 8 (over z, core), region: 4 (over y, x).
Axes of the slice: x: 2, y: 2, z: 4, core: 2. Of those that a mesh axis runs over, the one named last changes fastest.
Arguments:
- prior_states: bfloat16 [512, 65536], P('member', 'region'), may hold values from -6 to 6
- measured_values: bfloat16 [8192], P('region'), may hold values from -12 to 12
- measurement_precision: bfloat16 [8192], P('region'), may hold values from 0.5 to 4
- measured_subgrid_line: int32 [8192], P('region'), may hold values from 0 to 16383, as said below
- neighbour_measurement_lookup: int32 [4, 8, 1024], P('region'), may hold values from 0 to 6143, as said below
- active_entries_tally: int32 [4, 8], P('region', 'member'), may hold values from 512 to 1024, as said below
- distance_tier: int32 [4, 8, 1024], P('region', 'member'), may hold values from 0 to 8
- eastward_weight_share: int32 [4, 8, 2048], P('region', 'member'), may hold values from 0 to 8
Outputs:
- analysis: bfloat16 [512, 65536], P('member', 'region')
The draws below stay inside these ranges and needn't reach their ends.
Inputs may be any that keep to these rules, and one draw needn't show every extreme that they name: `neighbour_measurement_lookup`: for coarse point (s, p) the live and dead slots name distinct observations, all in blocks p-1, p, p+1 (each block 256 observations of a sector, in order) of sectors s-1, s, s+1; blocks outside 0 to 7 are never named. `measured_subgrid_line`: observation o of a sector measures a row of its block: from ((o % 2048) // 256) * 2048 to that plus 2048 - 1. `active_entries_tally`: some coarse point has all 1024 slots live.
All inputs are finite; a program needn't handle non-finite values.
Results may differ from the reference program's by a relative error of at most 0.019.
Values may be sent and summed in bfloat16 or wider, within the bound.
No kernel may reach another device: no remote copies, remote signals or barrier semaphores. Data moves between devices by JAX's collectives and lax.ppermute only.
A program may use at most 64 MiB of HBM per device.

```python
import math
import jax
import jax.numpy as jnp
from jax import lax

ENSEMBLE_SIZE = 512
LOC = 1024
ITERS = 6
OBS_CP = 256
SUBGRID_EACH = 2048
CP_TILE = 8
SECTORS = 4
OBS_ALL = 8192
SUBGRID_ALL = 65536
N_MEMBER = 8
N_REGION = 4


def draw_neighbour_measurement_lookup(key, part):
    latitude_swaths = N_MEMBER
    region_dimension = N_REGION
    obs_tile = OBS_CP * latitude_swaths
    cands = 9 * OBS_CP
    number = jnp.arange(cands, dtype=jnp.int32)
    side = number // (3 * OBS_CP)
    offset = number // OBS_CP % 3
    inside = number % OBS_CP
    coarse = jnp.arange(latitude_swaths, dtype=jnp.int32)[:, None]
    block = coarse + offset[None, :] - 1
    valid = (block >= 0) & (block < latitude_swaths)
    scores = jax.random.randint(key, (region_dimension, latitude_swaths, cands), 0, 65536) * cands + number
    scores = jnp.where(valid[None], scores, scores + 2 ** 30)
    order = jnp.argsort(scores, axis=-1, stable=True)[..., :LOC]
    table = side[None, :] * obs_tile + jnp.clip(block, 0, latitude_swaths - 1) * OBS_CP + inside[None, :]
    table = jnp.broadcast_to(table[None], (region_dimension, latitude_swaths, cands))
    return jnp.take_along_axis(table, order, axis=-1).astype(jnp.int32)


def draw_measured_subgrid_line(key, part):
    total = N_REGION * OBS_CP * N_MEMBER
    number = jnp.arange(total, dtype=jnp.int32)
    block = number % (OBS_CP * N_MEMBER) // OBS_CP
    return (block * SUBGRID_EACH + jax.random.randint(key, (total,), 0, SUBGRID_EACH)).astype(jnp.int32)


def draw_active_entries_tally(key, part):
    total = N_REGION * N_MEMBER
    counts = jax.random.randint(key, (total,), LOC // 2, LOC + 1)
    chosen_spot = jax.random.randint(jax.random.fold_in(key, 7), (), 0, total)
    counts = jnp.where(jnp.arange(total, dtype=jnp.int32) == chosen_spot, LOC, counts)
    return counts.reshape(N_REGION, N_MEMBER).astype(jnp.int32)


def with_ends(entries, key, least, largest):
    shape = entries.shape
    place = [jax.random.randint(jax.random.fold_in(key, axis), (), 0, shape[axis]) for axis in range(len(shape))]
    entries = entries.at[tuple(place)].set(least)
    longest = shape.index(max(shape))
    place[longest] = (place[longest] + 1) % shape[longest]
    return entries.at[tuple(place)].set(largest)


def steps_of(stream_key, shape, shards, low, top_value):
    gain = 1.0
    for axis_at, parts in shards:
        draws = jax.random.uniform(jax.random.fold_in(jax.random.fold_in(stream_key, 6), axis_at), (parts,), jnp.float32, low / len(shards), top_value / len(shards))
        gain = gain * jnp.repeat(jnp.exp(draws), shape[axis_at] // parts).reshape((-1,) + (1,) * (len(shape) - 1 - axis_at))
    return gain


def bell_draw(rng, extent, deviation, reach, split=(), kind=jnp.bfloat16):
    entries = deviation * jax.random.normal(rng, extent, jnp.float32)
    if split:
        entries = entries * steps_of(rng, extent, split, -0.22, 0.18)
    return jnp.clip(entries, -reach, reach).astype(kind)


def setup_inputs(seed: int = 0) -> dict:
    key_of = jax.random.split(jax.random.key(seed), 9)
    return {
        "prior_states": bell_draw(key_of[0], (ENSEMBLE_SIZE, SUBGRID_ALL), 1.0, 6.0, ((0, 8), (1, 4))),
        "measured_values": bell_draw(key_of[1], (OBS_ALL,), 2.0, 12.0, ((0, 4),)),
        "measurement_precision": jnp.clip(jnp.exp(math.log(4.0) - 2.0794415 * jax.random.uniform(key_of[2], (OBS_ALL,), jnp.float32) ** steps_of(key_of[2], (OBS_ALL,), ((0, 4),), -0.2, 0.2)), 0.5, 4.0).astype(jnp.bfloat16),
        "measured_subgrid_line": draw_measured_subgrid_line(jax.random.fold_in(key_of[8], 71), 0),
        "neighbour_measurement_lookup": draw_neighbour_measurement_lookup(jax.random.fold_in(key_of[8], 71), 0),
        "active_entries_tally": draw_active_entries_tally(jax.random.fold_in(key_of[8], 71), 0),
        "distance_tier": with_ends(jax.random.randint(key_of[6], (SECTORS, CP_TILE, LOC), 0, 9), jax.random.fold_in(key_of[6], 1), 0, 8).astype(jnp.int32),
        "eastward_weight_share": with_ends(jax.random.randint(key_of[7], (SECTORS, CP_TILE, SUBGRID_EACH), 0, 9), jax.random.fold_in(key_of[7], 1), 0, 8).astype(jnp.int32),
    }


def transform(chosen, obs_val, obs_w, count, dist):
    ensemble_dimension = chosen.shape[0]
    slots = chosen.shape[1]
    values = chosen.astype(jnp.float32)
    ybar = lax.optimization_barrier(jnp.mean(values, axis=0))
    pert = (values - ybar).astype(jnp.bfloat16)
    live = (jnp.arange(slots, dtype=jnp.int32) < count).astype(jnp.float32)
    wts = obs_w.astype(jnp.float32) * 2.0 / (2.0 + dist.astype(jnp.float32)) * live
    weighted = pert.astype(jnp.float32) * wts
    gram = lax.dot_general(weighted.astype(jnp.bfloat16), pert, (((1,), (1,)), ((), ())), preferred_element_type=jnp.float32)
    identity = jnp.eye(ensemble_dimension, dtype=jnp.float32)
    amat = gram + (ensemble_dimension - 1.0) * identity
    norm = jnp.sqrt(jnp.sum(amat * amat))
    gvec = jnp.dot(weighted, obs_val.astype(jnp.float32) - ybar, precision=lax.Precision.HIGHEST)
    zmat = (amat / norm).astype(jnp.bfloat16)
    ymat = identity.astype(jnp.bfloat16)
    for step in range(ITERS):
        product = jnp.dot(zmat, ymat, preferred_element_type=jnp.float32)
        tmat = (1.5 * identity - 0.5 * product).astype(jnp.bfloat16)
        ynext = jnp.dot(ymat, tmat, preferred_element_type=jnp.float32).astype(jnp.bfloat16)
        zmat = jnp.dot(tmat, zmat, preferred_element_type=jnp.float32).astype(jnp.bfloat16)
        ymat = ynext
    isq = ymat.astype(jnp.float32) / jnp.sqrt(norm)
    wbar = jnp.dot(isq, jnp.dot(isq, gvec, precision=lax.Precision.HIGHEST), precision=lax.Precision.HIGHEST)
    return (jnp.sqrt(ensemble_dimension - 1.0) * isq + wbar[:, None]).astype(jnp.bfloat16)

def update(vertical_dimension, weights, eastern, level):
    values = vertical_dimension.astype(jnp.float32)
    xbar = lax.optimization_barrier(jnp.mean(values, axis=0))
    centred = (values - xbar).astype(jnp.bfloat16)
    dims = (((0,), (0,)), ((), ()))
    own_term = lax.dot_general(weights, centred, dims, preferred_element_type=jnp.float32)
    east_term = lax.dot_general(eastern, centred, dims, preferred_element_type=jnp.float32)
    share = level.astype(jnp.float32) / 8.0
    return (xbar + (1.0 - share) * own_term + share * east_term).astype(jnp.bfloat16)

def reference(prior_states, measured_values, measurement_precision, measured_subgrid_line, neighbour_measurement_lookup, active_entries_tally, distance_tier, eastward_weight_share):
    region_dimension = N_REGION
    latitude_swaths = N_MEMBER
    obs_tile = OBS_CP * latitude_swaths
    fine_tile = SUBGRID_EACH * latitude_swaths
    sector_of = jnp.arange(region_dimension * obs_tile, dtype=jnp.int32) // obs_tile
    lateral_dimension = (sector_of * fine_tile + measured_subgrid_line).astype(jnp.int32)
    mapped_dimension = jnp.take(prior_states, lateral_dimension, axis=1)
    sector_ids = jnp.arange(region_dimension, dtype=jnp.int32)[:, None, None]
    side = neighbour_measurement_lookup // obs_tile
    within = neighbour_measurement_lookup % obs_tile
    global_idx = ((sector_ids + side - 1) % region_dimension * obs_tile + within).astype(jnp.int32)
    flat_idx = global_idx.reshape(region_dimension * latitude_swaths, LOC)

    def coarse(items):
        picks, count, dist = items
        chosen = jnp.take(mapped_dimension, picks, axis=1)
        return transform(chosen, measured_values[picks], measurement_precision[picks], count, dist)
    weights = lax.map(coarse, (flat_idx, active_entries_tally.reshape(region_dimension * latitude_swaths), distance_tier.reshape(region_dimension * latitude_swaths, LOC)))
    eastern = jnp.roll(weights.reshape(region_dimension, latitude_swaths, ENSEMBLE_SIZE, ENSEMBLE_SIZE), -1, axis=0).reshape(region_dimension * latitude_swaths, ENSEMBLE_SIZE, ENSEMBLE_SIZE)
    vertical_dimension = prior_states.reshape(ENSEMBLE_SIZE, region_dimension * latitude_swaths, SUBGRID_EACH).transpose(1, 0, 2)
    levels = eastward_weight_share.reshape(region_dimension * latitude_swaths, SUBGRID_EACH)

    def apply_rows(items):
        return update(items[0], items[1], items[2], items[3])
    result = lax.map(apply_rows, (vertical_dimension, weights, eastern, levels))
    return result.transpose(1, 0, 2).reshape(ENSEMBLE_SIZE, region_dimension * latitude_swaths * SUBGRID_EACH)
```

```python
import functools

import jax
import jax.numpy as jnp
from jax import lax
from jax.experimental import pallas as pl
from jax.experimental.pallas import tpu as pltpu
from jax.sharding import PartitionSpec as P

ITERS = 6

VMEM = pltpu.MemorySpace.VMEM
HBM = pltpu.MemorySpace.HBM


def nt_dot(a, b):
    return lax.dot_general(a, b, (((1,), (1,)), ((), ())), preferred_element_type=jnp.float32)


def partner(me, d, count):
    if count & (count - 1) == 0:
        return me ^ d
    return (me + d) % count


def source(me, d, count):
    if count & (count - 1) == 0:
        return me ^ d
    return (me + count - d) % count


def trade(value, d, count):
    pairs = [(i, partner(i, d, count)) for i in range(count)]
    return lax.ppermute(value, "member", pairs)


def gather_kernel(line_ref, x_ref, out_ref):
    rows = x_ref.shape[1]
    width = line_ref.shape[1]
    line = line_ref[...] - pl.program_id(0) * rows
    hot = (lax.broadcasted_iota(jnp.int32, (rows, width), 0) == line).astype(jnp.bfloat16)
    out_ref[0] = jnp.dot(x_ref[...], hot, preferred_element_type=jnp.float32).astype(jnp.bfloat16)


def gather_obs(prior, line, bands):
    members, fine = prior.shape
    rows = fine // bands
    width = line.shape[0] // bands
    return pl.pallas_call(
        gather_kernel,
        grid=(bands,),
        in_specs=[
            pl.BlockSpec((1, width), lambda b: (0, b)),
            pl.BlockSpec((members, rows), lambda b: (0, b)),
        ],
        out_specs=pl.BlockSpec((1, members, width), lambda b: (b, 0, 0)),
        out_shape=jax.ShapeDtypeStruct((bands, members, width), jnp.bfloat16),
        name="gather_obs",
    )(line.reshape(1, -1), prior)


def candidate_kernel(bands, count_ref, lookup_ref, dist_ref, low_ref, own_ref, high_ref, w_ref, val_ref):
    me = lax.axis_index("member")
    slots = lookup_ref.shape[1]
    obs_tile = own_ref.shape[1]
    width = obs_tile // bands
    index = lookup_ref[pl.ds(me, 1), :]
    live = lax.broadcasted_iota(jnp.int32, (1, slots), 1) < count_ref[0, 0]
    denom = jnp.where(live, 2.0 + dist_ref[...].astype(jnp.float32), 0.0)
    denom = jnp.broadcast_to(denom, (8, slots)).astype(jnp.bfloat16)
    rows = lax.broadcasted_iota(jnp.int32, (width, slots), 0)
    for off in range(3):
        band = me + off - 1
        valid = jnp.logical_and(band >= 0, band < bands)
        start = pl.multiple_of(jnp.clip(band, 0, bands - 1) * width, width)
        for side, ref in enumerate((low_ref, own_ref, high_ref)):
            base = jnp.where(valid, side * obs_tile + band * width, -4 * obs_tile)
            hot = (rows == index - base).astype(jnp.bfloat16)
            total = nt_dot(denom, hot)[0:1]
            pair = ref[:, pl.ds(start, width)].astype(jnp.float32)
            named = total > 0.0
            weight = pair[1:2] * 2.0 / jnp.where(named, total, 1.0)
            j = off * 3 + side
            w_ref[j : j + 1, :] = jnp.where(named, weight, 0.0)
            val_ref[j : j + 1, :] = pair[0:1]


def candidates(count, lookup, dist, low, own, high, bands):
    width = own.shape[1] // bands
    shape = jax.ShapeDtypeStruct((9, width), jnp.float32)
    return pl.pallas_call(
        functools.partial(candidate_kernel, bands),
        in_specs=[pl.BlockSpec(memory_space=pltpu.MemorySpace.SMEM)] + [pl.BlockSpec(memory_space=VMEM)] * 5,
        out_specs=[pl.BlockSpec(memory_space=VMEM)] * 2,
        out_shape=[shape, shape],
        name="candidates",
    )(count, lookup, dist, low, own, high)


def transform_kernel(before_ref, mid_ref, after_ref, w_ref, val_ref, out_ref, pert_ref, weighted_ref):
    members = out_ref.shape[0]
    width = w_ref.shape[1]
    gvec = jnp.zeros((members, 1), jnp.float32)
    for off, ref in enumerate((before_ref, mid_ref, after_ref)):
        for side in range(3):
            j = off * 3 + side
            values = ref[side].astype(jnp.float32)
            ybar = jnp.mean(values, axis=0, keepdims=True)
            pert = (values - ybar).astype(jnp.bfloat16)
            weighted = pert.astype(jnp.float32) * w_ref[j : j + 1, :]
            gvec = gvec + jnp.sum(weighted * (val_ref[j : j + 1, :] - ybar), axis=1, keepdims=True)
            pert_ref[:, j * width : (j + 1) * width] = pert
            weighted_ref[:, j * width : (j + 1) * width] = weighted.astype(jnp.bfloat16)
    gram = nt_dot(weighted_ref[...], pert_ref[...])
    row = lax.broadcasted_iota(jnp.int32, (members, members), 0)
    col = lax.broadcasted_iota(jnp.int32, (members, members), 1)
    eye = row == col
    amat = gram + jnp.where(eye, members - 1.0, 0.0)
    norm = jnp.sqrt(jnp.sum(jnp.sum(amat * amat, axis=1, keepdims=True), axis=0, keepdims=True))
    zmat = (amat / norm).astype(jnp.bfloat16)
    ident = jnp.where(eye, 1.5, 0.0)

    def mm(a, b):
        return jnp.dot(a, b, preferred_element_type=jnp.float32)

    tmat = (ident - 0.5 * zmat.astype(jnp.float32)).astype(jnp.bfloat16)
    ymat = tmat
    zmat = mm(tmat, zmat).astype(jnp.bfloat16)
    for step in range(1, ITERS):
        tmat = (ident - 0.5 * mm(zmat, ymat)).astype(jnp.bfloat16)
        ymat = mm(ymat, tmat).astype(jnp.bfloat16)
        if step < ITERS - 1:
            zmat = mm(tmat, zmat).astype(jnp.bfloat16)
    isq = ymat.astype(jnp.float32) / jnp.sqrt(norm)

    def as_row(column):
        return jnp.sum(jnp.where(eye, column, 0.0), axis=0, keepdims=True)

    once = jnp.sum(isq * as_row(gvec), axis=1, keepdims=True)
    wbar = jnp.sum(isq * as_row(once), axis=1, keepdims=True)
    out_ref[...] = (jnp.sqrt(members - 1.0) * isq + as_row(wbar)).astype(jnp.bfloat16)


def transform(before, mid, after, w, val):
    members = mid.shape[1]
    width = mid.shape[2]
    return pl.pallas_call(
        transform_kernel,
        in_specs=[pl.BlockSpec(memory_space=VMEM)] * 5,
        out_specs=pl.BlockSpec(memory_space=VMEM),
        out_shape=jax.ShapeDtypeStruct((members, members), jnp.bfloat16),
        scratch_shapes=[pltpu.VMEM((members, 9 * width), jnp.bfloat16)] * 2,
        name="transform",
    )(before, mid, after, w, val)


def update_kernel(count, wt_ref, we_ref, level_ref, *refs):
    ins, outs = refs[:count], refs[count : 2 * count]
    x_ref, y_ref, in_sem, out_sem = refs[2 * count :]
    me = lax.axis_index("member")
    each, rows = ins[1].shape
    members = each * count
    loads = []
    for d in range(count):
        to = x_ref.at[pl.ds(pl.multiple_of(source(me, d, count) * each, each), each), :]
        loads.append(pltpu.make_async_copy(ins[d], to, in_sem.at[d]))
        loads[-1].start()
    for load in loads:
        load.wait()
    step = min(rows, 512)
    for at in range(0, rows, step):
        cols = slice(at, at + step)
        values = x_ref[:, cols].astype(jnp.float32)
        xbar = jnp.mean(values, axis=0, keepdims=True)
        xp = (values - xbar).astype(jnp.bfloat16)
        own = jnp.dot(wt_ref[...], xp, preferred_element_type=jnp.float32)
        east = jnp.dot(we_ref[...], xp, preferred_element_type=jnp.float32)
        share = level_ref[:, cols].astype(jnp.float32) / 8.0
        y_ref[:, cols] = (xbar + (1.0 - share) * own + share * east).astype(jnp.bfloat16)
    stores = []
    for d in range(count):
        src = y_ref.at[pl.ds(pl.multiple_of(partner(me, d, count) * each, each), each), :]
        stores.append(pltpu.make_async_copy(src, outs[d], out_sem.at[d]))
        stores[-1].start()
    for store in stores:
        store.wait()


def update(wt, we, level, blocks):
    count = len(blocks)
    each, rows = blocks[0].shape
    return pl.pallas_call(
        functools.partial(update_kernel, count),
        in_specs=[pl.BlockSpec(memory_space=VMEM)] * 3 + [pl.BlockSpec(memory_space=HBM)] * count,
        out_specs=[pl.BlockSpec(memory_space=HBM)] * count,
        out_shape=[jax.ShapeDtypeStruct((each, rows), jnp.bfloat16)] * count,
        scratch_shapes=[
            pltpu.VMEM((each * count, rows), jnp.bfloat16),
            pltpu.VMEM((each * count, rows), jnp.bfloat16),
            pltpu.SemaphoreType.DMA((count,)),
            pltpu.SemaphoreType.DMA((count,)),
        ],
        name="update",
    )(wt, we, level, *blocks)


def assemble_kernel(count, *refs):
    ins, out_ref, sem = refs[:count], refs[count], refs[count + 1]
    me = lax.axis_index("member")
    rows = ins[0].shape[1]
    copies = []
    for d in range(count):
        to = out_ref.at[:, pl.ds(pl.multiple_of(source(me, d, count) * rows, rows), rows)]
        copies.append(pltpu.make_async_copy(ins[d], to, sem.at[d]))
        copies[-1].start()
    for copy in copies:
        copy.wait()


def assemble(blocks):
    count = len(blocks)
    each, rows = blocks[0].shape
    return pl.pallas_call(
        functools.partial(assemble_kernel, count),
        in_specs=[pl.BlockSpec(memory_space=HBM)] * count,
        out_specs=pl.BlockSpec(memory_space=HBM),
        out_shape=jax.ShapeDtypeStruct((each, rows * count), jnp.bfloat16),
        scratch_shapes=[pltpu.SemaphoreType.DMA((count,))],
        name="assemble",
    )(*blocks)


def local(
    prior_states,
    measured_values,
    measurement_precision,
    measured_subgrid_line,
    neighbour_measurement_lookup,
    active_entries_tally,
    distance_tier,
    eastward_weight_share,
):
    bands = lax.axis_size("member")
    sectors = lax.axis_size("region")
    me = lax.axis_index("member")
    each, fine = prior_states.shape
    rows = fine // bands
    east = [(i, (i + 1) % sectors) for i in range(sectors)]
    west = [(target, origin) for origin, target in east]
    north = [(i, i + 1) for i in range(bands - 1)]
    south = [(i + 1, i) for i in range(bands - 1)]

    paired = jnp.stack((measured_values, measurement_precision))
    pair_low = lax.ppermute(paired, "region", east)
    pair_high = lax.ppermute(paired, "region", west)

    proj = gather_obs(prior_states, measured_subgrid_line, bands)
    own = lax.all_to_all(proj, "member", split_axis=0, concat_axis=0, tiled=True)
    own = own.reshape(each * bands, -1)
    low = lax.ppermute(own, "region", east)
    high = lax.ppermute(own, "region", west)

    def block_for(d):
        return lax.dynamic_slice_in_dim(prior_states, partner(me, d, bands) * rows, rows, axis=1)

    states = [block_for(0)] + [trade(block_for(d), d, bands) for d in range(1, bands)]
    mid = jnp.stack((low, own, high))
    before = lax.ppermute(mid, "member", north)
    after = lax.ppermute(mid, "member", south)
    w, val = candidates(
        active_entries_tally, neighbour_measurement_lookup[0], distance_tier[0], pair_low, paired, pair_high, bands
    )
    wt = transform(before, mid, after, w, val)
    we = lax.ppermute(wt, "region", west)
    done = update(wt, we, eastward_weight_share[0], states)
    back = [done[0]] + [trade(done[d], d, bands) for d in range(1, bands)]
    return assemble(back)


def solution(mesh):
    in_specs = (
        P("member", "region"),
        P("region"),
        P("region"),
        P("region"),
        P("region", None, None),
        P("region", "member"),
        P("region", "member", None),
        P("region", "member", None),
    )
    out_specs = P("member", "region")
    return jax.shard_map(local, mesh=mesh, in_specs=in_specs, out_specs=out_specs, check_vma=False)
```

```python
import functools

import jax
import jax.numpy as jnp
from jax import lax
from jax.experimental import pallas as pl
from jax.experimental.pallas import tpu as pltpu
from jax.sharding import PartitionSpec as P


ITERS = 6

VMEM = pltpu.MemorySpace.VMEM
HBM = pltpu.MemorySpace.HBM


def nt_dot(a, b):
    return lax.dot_general(a, b, (((1,), (1,)), ((), ())), preferred_element_type=jnp.float32)


def partner(me, d, count):
    if count & (count - 1) == 0:
        return me ^ d
    return (me + d) % count


def source(me, d, count):
    if count & (count - 1) == 0:
        return me ^ d
    return (me + count - d) % count


def gather_kernel(line_ref, x_ref, out_ref):
    rows = x_ref.shape[1]
    width = line_ref.shape[1]
    line = line_ref[...] - pl.program_id(0) * rows
    hot = (lax.broadcasted_iota(jnp.int32, (rows, width), 0) == line).astype(jnp.bfloat16)
    out_ref[0] = jnp.dot(x_ref[...], hot, preferred_element_type=jnp.float32).astype(jnp.bfloat16)


def gather_obs(prior, line, bands):
    members, fine = prior.shape
    rows = fine // bands
    width = line.shape[0] // bands
    return pl.pallas_call(
        gather_kernel,
        grid=(bands,),
        in_specs=[
            pl.BlockSpec((1, width), lambda b: (0, b)),
            pl.BlockSpec((members, rows), lambda b: (0, b)),
        ],
        out_specs=pl.BlockSpec((1, members, width), lambda b: (b, 0, 0)),
        out_shape=jax.ShapeDtypeStruct((bands, members, width), jnp.bfloat16),
        name="gather_obs",
    )(line.reshape(1, -1), prior)


def candidate_kernel(bands, count_ref, lookup_ref, dist_ref, low_ref, own_ref, high_ref, w_ref, val_ref):
    me = lax.axis_index("member")
    slots = lookup_ref.shape[1]
    obs_tile = own_ref.shape[1]
    width = obs_tile // bands
    index = lookup_ref[pl.ds(me, 1), :]
    live = lax.broadcasted_iota(jnp.int32, (1, slots), 1) < count_ref[0, 0]
    denom = jnp.where(live, 2.0 + dist_ref[...].astype(jnp.float32), 0.0)
    denom = jnp.broadcast_to(denom, (8, slots)).astype(jnp.bfloat16)
    rows = lax.broadcasted_iota(jnp.int32, (width, slots), 0)
    for off in range(3):
        band = me + off - 1
        valid = jnp.logical_and(band >= 0, band < bands)
        start = pl.multiple_of(jnp.clip(band, 0, bands - 1) * width, width)
        for side, ref in enumerate((low_ref, own_ref, high_ref)):
            base = jnp.where(valid, side * obs_tile + band * width, -4 * obs_tile)
            hot = (rows == index - base).astype(jnp.bfloat16)
            total = nt_dot(denom, hot)[0:1]
            pair = ref[:, pl.ds(start, width)].astype(jnp.float32)
            named = total > 0.0
            weight = pair[1:2] * 2.0 / jnp.where(named, total, 1.0)
            j = off * 3 + side
            w_ref[j : j + 1, :] = jnp.where(named, weight, 0.0)
            val_ref[j : j + 1, :] = pair[0:1]


def candidates(count, lookup, dist, low, own, high, bands):
    width = own.shape[1] // bands
    shape = jax.ShapeDtypeStruct((9, width), jnp.float32)
    return pl.pallas_call(
        functools.partial(candidate_kernel, bands),
        in_specs=[pl.BlockSpec(memory_space=pltpu.MemorySpace.SMEM)] + [pl.BlockSpec(memory_space=VMEM)] * 5,
        out_specs=[pl.BlockSpec(memory_space=VMEM)] * 2,
        out_shape=[shape, shape],
        name="candidates",
    )(count, lookup, dist, low, own, high)


def transform_kernel(
    count, before_ref, mid_ref, after_ref, w_ref, val_ref, near_ref, far_ref, pert_ref, weighted_ref, wt_ref
):
    members = wt_ref.shape[0]
    width = w_ref.shape[1]
    gvec = jnp.zeros((members, 1), jnp.float32)
    for off, ref in enumerate((before_ref, mid_ref, after_ref)):
        for side in range(3):
            j = off * 3 + side
            values = ref[side].astype(jnp.float32)
            ybar = jnp.mean(values, axis=0, keepdims=True)
            pert = (values - ybar).astype(jnp.bfloat16)
            weighted = pert.astype(jnp.float32) * w_ref[j : j + 1, :]
            gvec = gvec + jnp.sum(weighted * (val_ref[j : j + 1, :] - ybar), axis=1, keepdims=True)
            pert_ref[:, j * width : (j + 1) * width] = pert
            weighted_ref[:, j * width : (j + 1) * width] = weighted.astype(jnp.bfloat16)
    gram = nt_dot(weighted_ref[...], pert_ref[...])
    row = lax.broadcasted_iota(jnp.int32, (members, members), 0)
    col = lax.broadcasted_iota(jnp.int32, (members, members), 1)
    eye = row == col
    amat = gram + jnp.where(eye, members - 1.0, 0.0)
    norm = jnp.sqrt(jnp.sum(jnp.sum(amat * amat, axis=1, keepdims=True), axis=0, keepdims=True))
    zmat = (amat / norm).astype(jnp.bfloat16)
    ident = jnp.where(eye, 1.5, 0.0)

    def mm(a, b):
        return jnp.dot(a, b, preferred_element_type=jnp.float32)

    tmat = (ident - 0.5 * zmat.astype(jnp.float32)).astype(jnp.bfloat16)
    ymat = tmat
    zmat = mm(tmat, zmat).astype(jnp.bfloat16)
    for step in range(1, ITERS):
        tmat = (ident - 0.5 * mm(zmat, ymat)).astype(jnp.bfloat16)
        ymat = mm(ymat, tmat).astype(jnp.bfloat16)
        if step < ITERS - 1:
            zmat = mm(tmat, zmat).astype(jnp.bfloat16)
    isq = ymat.astype(jnp.float32) / jnp.sqrt(norm)

    def as_row(column):
        return jnp.sum(jnp.where(eye, column, 0.0), axis=0, keepdims=True)

    once = jnp.sum(isq * as_row(gvec), axis=1, keepdims=True)
    wbar = jnp.sum(isq * as_row(once), axis=1, keepdims=True)
    wt_ref[...] = (jnp.sqrt(members - 1.0) * isq + as_row(wbar)).astype(jnp.bfloat16)
    me = lax.axis_index("member")
    each = members // count
    half = count // 2
    for d in range(count):
        rows = wt_ref[pl.ds(pl.multiple_of(partner(me, d, count) * each, each), each), :]
        if d < half:
            near_ref[d * each : (d + 1) * each, :] = rows
        else:
            far_ref[(d - half) * each : (d - half + 1) * each, :] = rows


def transform(before, mid, after, w, val, count):
    members = mid.shape[1]
    width = mid.shape[2]
    each = members // count
    half = count // 2
    return pl.pallas_call(
        functools.partial(transform_kernel, count),
        in_specs=[pl.BlockSpec(memory_space=VMEM)] * 5,
        out_specs=[pl.BlockSpec(memory_space=VMEM)] * 2,
        out_shape=[
            jax.ShapeDtypeStruct((half * each, members), jnp.bfloat16),
            jax.ShapeDtypeStruct(((count - half) * each, members), jnp.bfloat16),
        ],
        scratch_shapes=[
            pltpu.VMEM((members, 9 * width), jnp.bfloat16),
            pltpu.VMEM((members, 9 * width), jnp.bfloat16),
            pltpu.VMEM((members, members), jnp.bfloat16),
        ],
        name="transform",
    )(before, mid, after, w, val)


def analysis(wt_ref, we_ref, level_ref, xbar, xp, cols, outs):
    own = jnp.dot(wt_ref[...], xp, preferred_element_type=jnp.float32)
    east = jnp.dot(we_ref[...], xp, preferred_element_type=jnp.float32)
    share = level_ref[:, cols].astype(jnp.float32) / 8.0
    result = (xbar + (1.0 - share) * own + share * east).astype(jnp.bfloat16)
    each = outs[0].shape[0]
    for place, out in enumerate(outs):
        out[:, cols] = result[place * each : (place + 1) * each]


def far_kernel(count, wt_ref, we_ref, level_ref, *refs):
    ins, xbar_ref, xp_ref, outs = refs[:count], refs[count], refs[count + 1], refs[count + 2 : -2]
    x_ref, sem = refs[-2:]
    me = lax.axis_index("member")
    each, rows = ins[1].shape
    loads = []
    for d in range(count):
        to = x_ref.at[pl.ds(pl.multiple_of(source(me, d, count) * each, each), each), :]
        loads.append(pltpu.make_async_copy(ins[d], to, sem.at[d]))
        loads[-1].start()
    for load in loads:
        load.wait()
    step = min(rows, 512)
    for at in range(0, rows, step):
        cols = slice(at, at + step)
        values = x_ref[:, cols].astype(jnp.float32)
        xbar = jnp.mean(values, axis=0, keepdims=True)
        xp = (values - xbar).astype(jnp.bfloat16)
        xbar_ref[:, cols] = xbar
        xp_ref[:, cols] = xp
        analysis(wt_ref, we_ref, level_ref, xbar, xp, cols, outs)


def far_update(wt, we, level, blocks):
    count = len(blocks)
    each, rows = blocks[0].shape
    members = each * count
    part = wt.shape[0] // each
    return pl.pallas_call(
        functools.partial(far_kernel, count),
        in_specs=[pl.BlockSpec(memory_space=VMEM)] * 3 + [pl.BlockSpec(memory_space=HBM)] * count,
        out_specs=[pl.BlockSpec(memory_space=VMEM)] * (2 + part),
        out_shape=[
            jax.ShapeDtypeStruct((1, rows), jnp.float32),
            jax.ShapeDtypeStruct((members, rows), jnp.bfloat16),
        ]
        + [jax.ShapeDtypeStruct((each, rows), jnp.bfloat16)] * part,
        scratch_shapes=[pltpu.VMEM((members, rows), jnp.bfloat16), pltpu.SemaphoreType.DMA((count,))],
        name="far_update",
    )(wt, we, level, *blocks)


def near_kernel(wt_ref, we_ref, level_ref, xbar_ref, xp_ref, *outs):
    rows = xp_ref.shape[1]
    step = min(rows, 512)
    for at in range(0, rows, step):
        cols = slice(at, at + step)
        analysis(wt_ref, we_ref, level_ref, xbar_ref[:, cols], xp_ref[:, cols], cols, outs)


def near_update(wt, we, level, xbar, xp, each):
    rows = xp.shape[1]
    part = wt.shape[0] // each
    return pl.pallas_call(
        near_kernel,
        in_specs=[pl.BlockSpec(memory_space=VMEM)] * 5,
        out_specs=[pl.BlockSpec(memory_space=VMEM)] * part,
        out_shape=[jax.ShapeDtypeStruct((each, rows), jnp.bfloat16)] * part,
        name="near_update",
    )(wt, we, level, xbar, xp)


def assemble_kernel(count, *refs):
    ins, out_ref, sem = refs[:count], refs[count], refs[count + 1]
    me = lax.axis_index("member")
    rows = ins[0].shape[1]
    copies = []
    for d in range(count):
        to = out_ref.at[:, pl.ds(pl.multiple_of(source(me, d, count) * rows, rows), rows)]
        copies.append(pltpu.make_async_copy(ins[d], to, sem.at[d]))
        copies[-1].start()
    for copy in copies:
        copy.wait()


def assemble(blocks):
    count = len(blocks)
    each, rows = blocks[0].shape
    return pl.pallas_call(
        functools.partial(assemble_kernel, count),
        in_specs=[pl.BlockSpec(memory_space=VMEM)] * count,
        out_specs=pl.BlockSpec(memory_space=HBM),
        out_shape=jax.ShapeDtypeStruct((each, rows * count), jnp.bfloat16),
        scratch_shapes=[pltpu.SemaphoreType.DMA((count,))],
        name="assemble",
    )(*blocks)


def local(
    prior_states,
    measured_values,
    measurement_precision,
    measured_subgrid_line,
    neighbour_measurement_lookup,
    active_entries_tally,
    distance_tier,
    eastward_weight_share,
):
    bands = lax.axis_size("member")
    sectors = lax.axis_size("region")
    me = lax.axis_index("member")
    each, fine = prior_states.shape
    rows = fine // bands
    east = [(i, (i + 1) % sectors) for i in range(sectors)]
    west = [(target, origin) for origin, target in east]
    north = [(i, i + 1) for i in range(bands - 1)]
    south = [(i + 1, i) for i in range(bands - 1)]

    half = bands // 2

    def block_for(d):
        return lax.dynamic_slice_in_dim(prior_states, partner(me, d, bands) * rows, rows, axis=1)

    def trade(value, d):
        return lax.ppermute(value, "member", [(i, partner(i, d, bands)) for i in range(bands)])

    states = [block_for(0)] + [trade(block_for(d), d) for d in range(1, bands)]
    paired = jnp.stack((measured_values, measurement_precision))
    pair_low = lax.ppermute(paired, "region", east)
    pair_high = lax.ppermute(paired, "region", west)

    proj = gather_obs(prior_states, measured_subgrid_line, bands)
    own = lax.all_to_all(proj, "member", split_axis=0, concat_axis=0, tiled=True)
    own = own.reshape(each * bands, -1)
    low = lax.ppermute(own, "region", east)
    high = lax.ppermute(own, "region", west)
    mid = jnp.stack((low, own, high))
    before = lax.ppermute(mid, "member", north)
    after = lax.ppermute(mid, "member", south)
    w, val = candidates(
        active_entries_tally, neighbour_measurement_lookup[0], distance_tier[0], pair_low, paired, pair_high, bands
    )
    wt_near, wt_far = transform(before, mid, after, w, val, bands)
    we_far = lax.ppermute(wt_far, "region", west)
    we_near = lax.ppermute(wt_near, "region", west)
    level = eastward_weight_share[0]
    xbar, xp, *far = far_update(wt_far, we_far, level, states)
    back_far = [trade(far[d - half], d) for d in range(half, bands)]
    near = near_update(wt_near, we_near, level, xbar, xp, each)
    back_near = [near[0]] + [trade(near[d], d) for d in range(1, half)]
    return assemble(back_near + back_far)


def solution(mesh):
    in_specs = (
        P("member", "region"),
        P("region"),
        P("region"),
        P("region"),
        P("region", None, None),
        P("region", "member"),
        P("region", "member", None),
        P("region", "member", None),
    )
    out_specs = P("member", "region")
    return jax.shard_map(local, mesh=mesh, in_specs=in_specs, out_specs=out_specs, check_vma=False)
```

```python
import functools

import jax
import jax.numpy as jnp
from jax import lax
from jax.experimental import pallas as pl
from jax.experimental.pallas import tpu as pltpu
from jax.sharding import PartitionSpec as P


ITERS = 6

VMEM = pltpu.MemorySpace.VMEM
GRANT = pltpu.CompilerParams(vmem_limit_bytes=20 * 2**20)


def nt_dot(a, b):
    return lax.dot_general(a, b, (((1,), (1,)), ((), ())), preferred_element_type=jnp.float32)


def partner(me, d, count):
    if count & (count - 1) == 0:
        return me ^ d
    return (me + d) % count


def twin(me):
    return me + 1 - 2 * (me % 2)


def neighbour(me):
    return me - 1 + 2 * (me % 2)


def source(me, d, count):
    if count & (count - 1) == 0:
        return me ^ d
    return (me + count - d) % count


def gather_kernel(width, line_ref, x_ref, out_ref):
    group, members, _ = out_ref.shape
    rows = x_ref.shape[1] // group
    chunks = rows // width
    for g in range(group):
        line = line_ref[:, g * width : (g + 1) * width] - (pl.program_id(0) * group + g) * rows
        chunk = line // width
        place = line - chunk * width
        hot = (lax.broadcasted_iota(jnp.int32, (width, width), 0) == place).astype(jnp.bfloat16)
        at = g * rows
        stack = jnp.concatenate([x_ref[:, at + c * width : at + (c + 1) * width] for c in range(chunks)], axis=0)
        picked = jnp.dot(stack, hot, preferred_element_type=jnp.float32)
        result = picked[:members]
        for c in range(1, chunks):
            result = jnp.where(chunk == c, picked[c * members : (c + 1) * members], result)
        out_ref[g] = result.astype(jnp.bfloat16)


def gather_obs(prior, line, bands):
    members, fine = prior.shape
    rows = fine // bands
    width = line.shape[0] // bands
    group = 2 if bands % 2 == 0 else 1
    return pl.pallas_call(
        functools.partial(gather_kernel, width),
        grid=(bands // group,),
        in_specs=[
            pl.BlockSpec((1, group * width), lambda b: (0, b)),
            pl.BlockSpec((members, group * rows), lambda b: (0, b)),
        ],
        out_specs=pl.BlockSpec((group, members, width), lambda b: (b, 0, 0)),
        out_shape=jax.ShapeDtypeStruct((bands, members, width), jnp.bfloat16),
        name="gather_obs",
        compiler_params=GRANT,
    )(line.reshape(1, -1), prior)


def candidate_kernel(bands, count_ref, lookup_ref, dist_ref, low_ref, own_ref, high_ref, w_ref, val_ref):
    me = lax.axis_index("member")
    slots = lookup_ref.shape[1]
    obs_tile = own_ref.shape[1]
    width = obs_tile // bands
    index = lookup_ref[pl.ds(me, 1), :]
    live = lax.broadcasted_iota(jnp.int32, (1, slots), 1) < count_ref[0, 0]
    denom = jnp.where(live, 2.0 + dist_ref[...].astype(jnp.float32), 0.0)
    denom = jnp.broadcast_to(denom, (8, slots)).astype(jnp.bfloat16)
    rows = lax.broadcasted_iota(jnp.int32, (width, slots), 0)
    for off, band in enumerate((me, twin(me), neighbour(me))):
        valid = jnp.logical_and(band >= 0, band < bands)
        start = pl.multiple_of(jnp.clip(band, 0, bands - 1) * width, width)
        for side, ref in enumerate((low_ref, own_ref, high_ref)):
            base = jnp.where(valid, side * obs_tile + band * width, -4 * obs_tile)
            hot = (rows == index - base).astype(jnp.bfloat16)
            total = nt_dot(denom, hot)[0:1]
            pair = ref[:, pl.ds(start, width)].astype(jnp.float32)
            named = total > 0.0
            weight = pair[1:2] * 2.0 / jnp.where(named, total, 1.0)
            j = off * 3 + side
            w_ref[j : j + 1, :] = jnp.where(named, weight, 0.0)
            val_ref[j : j + 1, :] = pair[0:1]


def candidates(count, lookup, dist, low, own, high, bands):
    width = own.shape[1] // bands
    shape = jax.ShapeDtypeStruct((9, width), jnp.float32)
    return pl.pallas_call(
        functools.partial(candidate_kernel, bands),
        in_specs=[pl.BlockSpec(memory_space=pltpu.MemorySpace.SMEM)] + [pl.BlockSpec(memory_space=VMEM)] * 5,
        out_specs=[pl.BlockSpec(memory_space=VMEM)] * 2,
        out_shape=[shape, shape],
        name="candidates",
        compiler_params=GRANT,
    )(count, lookup, dist, low, own, high)


def as_row(column, eye):
    return jnp.sum(jnp.where(eye, column, 0.0), axis=0, keepdims=True)


def eye_mask(members):
    row = lax.broadcasted_iota(jnp.int32, (members, members), 0)
    return row == lax.broadcasted_iota(jnp.int32, (members, members), 1)


def add_planes(planes, places, w_ref, val_ref, pert_ref, weighted_ref):
    members, width = planes[0].shape
    gvec = jnp.zeros((members, 1), jnp.float32)
    for at, (j, ref) in enumerate(zip(places, planes)):
        values = ref[...].astype(jnp.float32)
        ybar = jnp.mean(values, axis=0, keepdims=True)
        pert = (values - ybar).astype(jnp.bfloat16)
        weighted = pert.astype(jnp.float32) * w_ref[j : j + 1, :]
        gvec = gvec + jnp.sum(weighted * (val_ref[j : j + 1, :] - ybar), axis=1, keepdims=True)
        pert_ref[:, at * width : (at + 1) * width] = pert
        weighted_ref[:, at * width : (at + 1) * width] = weighted.astype(jnp.bfloat16)
    return nt_dot(weighted_ref[...], pert_ref[...]), gvec


def gram_kernel(places, *refs):
    planes, (w_ref, val_ref, gram_ref, gvec_ref, pert_ref, weighted_ref) = refs[:-6], refs[-6:]
    gram, gvec = add_planes(planes, places, w_ref, val_ref, pert_ref, weighted_ref)
    gram_ref[...] = gram
    gvec_ref[...] = as_row(gvec, eye_mask(gram.shape[0]))


def gram_part(planes, places, w, val):
    members, width = planes[0].shape
    return pl.pallas_call(
        functools.partial(gram_kernel, places),
        in_specs=[pl.BlockSpec(memory_space=VMEM)] * (len(planes) + 2),
        out_specs=[pl.BlockSpec(memory_space=VMEM)] * 2,
        out_shape=[
            jax.ShapeDtypeStruct((members, members), jnp.float32),
            jax.ShapeDtypeStruct((1, members), jnp.float32),
        ],
        scratch_shapes=[pltpu.VMEM((members, len(planes) * width), jnp.bfloat16)] * 2,
        name="gram_part",
        compiler_params=GRANT,
    )(*planes, w, val)


def transform_kernel(
    count, places, before_ref, after_ref, w_ref, val_ref, gram_ref, part_ref, near_ref, far_ref, pert_ref, weighted_ref, wt_ref
):
    members = wt_ref.shape[0]
    planes = (before_ref.at[0], before_ref.at[1], after_ref.at[0], after_ref.at[1])
    gram, gvec = add_planes(planes, places, w_ref, val_ref, pert_ref, weighted_ref)
    eye = eye_mask(members)
    amat = gram_ref[...] + gram + jnp.where(eye, members - 1.0, 0.0)
    norm = jnp.sqrt(jnp.sum(jnp.sum(amat * amat, axis=1, keepdims=True), axis=0, keepdims=True))
    zmat = (amat / norm).astype(jnp.bfloat16)
    ident = jnp.where(eye, 1.5, 0.0)

    def mm(a, b):
        return jnp.dot(a, b, preferred_element_type=jnp.float32)

    tmat = (ident - 0.5 * zmat.astype(jnp.float32)).astype(jnp.bfloat16)
    ymat = tmat
    zmat = mm(tmat, zmat).astype(jnp.bfloat16)
    for step in range(1, ITERS):
        tmat = (ident - 0.5 * mm(zmat, ymat)).astype(jnp.bfloat16)
        ymat = mm(ymat, tmat).astype(jnp.bfloat16)
        if step < ITERS - 1:
            zmat = mm(tmat, zmat).astype(jnp.bfloat16)
    isq = ymat.astype(jnp.float32) / jnp.sqrt(norm)
    once = jnp.sum(isq * (part_ref[...] + as_row(gvec, eye)), axis=1, keepdims=True)
    wbar = jnp.sum(isq * as_row(once, eye), axis=1, keepdims=True)
    wt_ref[...] = (jnp.sqrt(members - 1.0) * isq + as_row(wbar, eye)).astype(jnp.bfloat16)
    me = lax.axis_index("member")
    each = members // count
    half = count // 2
    for d in range(count):
        rows = wt_ref[pl.ds(pl.multiple_of(partner(me, d, count) * each, each), each), :]
        if d < half:
            near_ref[d * each : (d + 1) * each, :] = rows
        else:
            far_ref[(d - half) * each : (d - half + 1) * each, :] = rows


def transform(before, after, places, w, val, gram, gvec, count):
    _, members, width = before.shape
    each = members // count
    half = count // 2
    return pl.pallas_call(
        functools.partial(transform_kernel, count, places),
        in_specs=[pl.BlockSpec(memory_space=VMEM)] * 6,
        out_specs=[pl.BlockSpec(memory_space=VMEM)] * 2,
        out_shape=[
            jax.ShapeDtypeStruct((half * each, members), jnp.bfloat16),
            jax.ShapeDtypeStruct(((count - half) * each, members), jnp.bfloat16),
        ],
        scratch_shapes=[
            pltpu.VMEM((members, len(places) * width), jnp.bfloat16),
            pltpu.VMEM((members, len(places) * width), jnp.bfloat16),
            pltpu.VMEM((members, members), jnp.bfloat16),
        ],
        name="transform",
        compiler_params=GRANT,
    )(before, after, w, val, gram, gvec)


def update_kernel(count, step, wt_ref, we_ref, level_ref, *refs):
    ins, outs, x_ref = refs[:count], refs[count:-1], refs[-1]
    me = lax.axis_index("member")
    each, rows = ins[1].shape
    members = each * count
    for d, ref in enumerate(ins):
        x_ref[pl.ds(pl.multiple_of(source(me, d, count) * each, each), each), :] = ref[...]
    own_sum = jnp.sum(wt_ref[...].astype(jnp.float32), axis=1, keepdims=True)
    east_sum = jnp.sum(we_ref[...].astype(jnp.float32), axis=1, keepdims=True)
    ones = jnp.ones((8, members), jnp.bfloat16)
    for at in range(0, rows, step):
        cols = slice(at, at + step)
        x = x_ref[:, cols]
        xbar = jnp.dot(ones, x, preferred_element_type=jnp.float32)[0:1] * (1.0 / members)
        own = jnp.dot(wt_ref[...], x, preferred_element_type=jnp.float32) - own_sum * xbar
        east = jnp.dot(we_ref[...], x, preferred_element_type=jnp.float32) - east_sum * xbar
        share = level_ref[:, cols].astype(jnp.float32) / 8.0
        result = (xbar + (1.0 - share) * own + share * east).astype(jnp.bfloat16)
        for place, out in enumerate(outs):
            out[:, cols] = result[place * each : (place + 1) * each]


def update(wt, we, level, blocks):
    count = len(blocks)
    each, rows = blocks[0].shape
    part = wt.shape[0] // each
    step = min(rows, 512)
    return pl.pallas_call(
        functools.partial(update_kernel, count, step),
        in_specs=[pl.BlockSpec(memory_space=VMEM)] * (3 + count),
        out_specs=[pl.BlockSpec(memory_space=VMEM)] * part,
        out_shape=[jax.ShapeDtypeStruct((each, rows), jnp.bfloat16)] * part,
        scratch_shapes=[pltpu.VMEM((each * count, rows), jnp.bfloat16)],
        compiler_params=GRANT,
    )(wt, we, level, *blocks)


def local(
    prior_states,
    measured_values,
    measurement_precision,
    measured_subgrid_line,
    neighbour_measurement_lookup,
    active_entries_tally,
    distance_tier,
    eastward_weight_share,
):
    bands = lax.axis_size("member")
    sectors = lax.axis_size("region")
    me = lax.axis_index("member")
    each, fine = prior_states.shape
    rows = fine // bands
    east = [(i, (i + 1) % sectors) for i in range(sectors)]
    west = [(target, origin) for origin, target in east]
    twins = [(i, twin(i)) for i in range(bands) if twin(i) < bands]
    other = [(i, neighbour(i)) for i in range(bands) if 0 <= neighbour(i) < bands]

    half = bands // 2

    def block_for(prior, d):
        return lax.dynamic_slice_in_dim(prior, partner(me, d, bands) * rows, rows, axis=1)

    def trade(value, d):
        return lax.ppermute(value, "member", [(i, partner(i, d, bands)) for i in range(bands)])

    def after(value, *others):
        return lax.optimization_barrier((value, *others))[0]

    first, middle, last = groups(bands)
    blocks = {d: block_for(prior_states, d) for d in first}
    states = {d: trade(blocks[d], d) for d in first}
    paired = jnp.stack((measured_values, measurement_precision))
    proj = gather_obs(prior_states, measured_subgrid_line, bands)
    prior_later = after(prior_states, proj)
    blocks.update({d: block_for(prior_later, d) for d in [0, *middle, *last]})
    own = lax.all_to_all(proj, "member", split_axis=0, concat_axis=0, tiled=True)
    own = own.reshape(each * bands, -1)
    pair_low = lax.ppermute(paired, "region", east)
    pair_high = lax.ppermute(paired, "region", west)
    states[0] = blocks[0]
    for d in middle:
        states[d] = trade(after(blocks[d], own), d)
    low = lax.ppermute(own, "region", east)
    high = lax.ppermute(own, "region", west)
    own_n = lax.ppermute(own, "member", other)
    own_t = lax.ppermute(own, "member", twins)
    sides = jnp.stack((low, high))
    sides_n = lax.ppermute(sides, "member", other)
    sides_t = lax.ppermute(sides, "member", twins)
    for d in last:
        states[d] = trade(after(blocks[d], sides_n, sides_t), d)
    w, val = candidates(
        active_entries_tally, neighbour_measurement_lookup[0], distance_tier[0], pair_low, paired, pair_high, bands
    )
    gram, gvec = gram_part((low, own, high, own_t, own_n), (0, 1, 2, 4, 7), w, val)
    wt_near, wt_far = transform(sides_t, sides_n, (3, 5, 6, 8), w, val, gram, gvec, bands)
    we_far = lax.ppermute(wt_far, "region", west)
    we_near = lax.ppermute(wt_near, "region", west)
    level = eastward_weight_share[0]
    ordered = [states[d] for d in range(bands)]
    far = update(wt_far, we_far, level, ordered)
    back = {d: trade(far[d - half], d) for d in range(half, bands)}
    near = update(wt_near, we_near, level, ordered)
    back[0] = near[0]
    for d in range(1, half):
        back[d] = trade(near[d], d)
    result = jnp.zeros((each, fine), jnp.bfloat16)
    for d in [0, *range(half, bands), *range(1, half)]:
        result = lax.dynamic_update_slice_in_dim(result, back[d], source(me, d, bands) * rows, axis=1)
    return result


def groups(bands):
    half = bands // 2
    quarter = max(half // 4, 1)
    far = list(range(half, bands))
    near = list(range(2, half))
    cut = len(near) // 2
    middle = far[quarter : 2 * quarter] + near[:cut] + list(range(1, min(2, half)))
    return far[:quarter], middle, far[2 * quarter :] + near[cut:]


def solution(mesh):
    in_specs = (
        P("member", "region"),
        P("region"),
        P("region"),
        P("region"),
        P("region", None, None),
        P("region", "member"),
        P("region", "member", None),
        P("region", "member", None),
    )
    out_specs = P("member", "region")
    return jax.shard_map(local, mesh=mesh, in_specs=in_specs, out_specs=out_specs, check_vma=False)
```
